32 devices in a mesh: row: 4 (over y, x), col: 8 (over z, core).
Axes of the slice: x: 2, y: 2, z: 4, core: 2. Of those that a mesh axis runs over, the one named last changes fastest.
Arguments:
- pair_rep: bfloat16 [512, 512, 128], P('row', 'col'), may hold values from -6 to 6
- ln_gain: float32 [128], replicated, may hold values from 0.1 to 1.9
- ln_shift: float32 [128], replicated, may hold values from -3 to 3
- w_proj: bfloat16 [128, 512], replicated, may hold values from -0.5 to 0.5
- gate_bias: float32 [128], replicated, may hold values from -4 to 4
- w_bias: bfloat16 [128, 4], replicated, may hold values from -11 to 11
- w_out: bfloat16 [128, 128], replicated, may hold values from -0.5 to 0.5
- out_bias: float32 [128], replicated, may hold values from -3 to 3
- block_valid: int32 [4], replicated, may hold values from 0 to 1, as said below
Outputs:
- pair_out: bfloat16 [512, 512, 128], P('row', 'col')
The draws below stay inside these ranges and needn't reach their ends.
Inputs may be any that keep to these rules, and one draw needn't show every extreme that they name: block_valid[b] is 1 when residues b * 128 to (b + 1) * 128 - 1 are present and 0 when they are padding; blocks 0 and 2 are always present, and at least one other block is always padding.
All inputs are finite; a program needn't handle non-finite values.
Results may differ from the reference program's by a relative error of at most 0.0082.
Values may be sent and summed in bfloat16 or wider, within the bound.
A program may use at most 192 MiB of HBM per device.

```python
import jax
import jax.numpy as jnp
from jax import lax

C = 128
H = 4
HD = 32
RES = 512
NBLK = 4


def draw_w_bias(key, part):
    base = jnp.clip(jax.random.normal(key, (C, H), jnp.float32), -4.0, 4.0) * 0.13
    return base.astype(jnp.bfloat16)


def draw_block_valid(key, part):
    places = jnp.arange(NBLK, dtype=jnp.int32)
    levels = jax.random.randint(key, (NBLK,), 0, 2, dtype=jnp.int32)
    bits = jnp.where(levels > 0, 1, 0).astype(jnp.int32)
    bits = jnp.where((places == 0) | (places == NBLK // 2), 1, bits)
    if NBLK >= 3:
        candidate = jax.random.randint(jax.random.fold_in(key, 7), (), 1, NBLK - 1, dtype=jnp.int32)
        padded = jnp.where(candidate == NBLK // 2, NBLK - 1, candidate).astype(jnp.int32)
        bits = jnp.where(places == padded, 0, bits)
    return bits.astype(jnp.int32)


def level_of(own_key, dims, pieces, low, high):
    level = 1.0
    for dim, blocks in pieces:
        steps = jax.random.uniform(jax.random.fold_in(jax.random.fold_in(own_key, 6), dim), (blocks,), jnp.float32, low / len(pieces), high / len(pieces))
        level = level * jnp.repeat(jnp.exp(steps), dims[dim] // blocks).reshape((-1,) + (1,) * (len(dims) - 1 - dim))
    return level


def noise(rng, dims, deviation, most, split=(), kind=jnp.bfloat16):
    gain = level_of(rng, dims, split, -0.22, 0.18) if split else 1.0
    values = jax.random.normal(rng, dims, jnp.float32) * deviation * gain
    return jnp.minimum(jnp.maximum(values, -most), most).astype(kind)


def setup_inputs(seed: int = 0) -> dict:
    arg_keys = jax.random.split(jax.random.key(seed), 10)
    return {
        "pair_rep": noise(arg_keys[0], (RES, RES, C), 1.0, 6.0, ((0, 4), (1, 8))),
        "ln_gain": jnp.clip(1.0 + 0.18 * jax.random.normal(arg_keys[1], (C,), jnp.float32), 0.1, 1.9),
        "ln_shift": noise(arg_keys[2], (C,), 0.5, 3.0, (), jnp.float32),
        "w_proj": noise(arg_keys[3], (C, 4 * H * HD), C ** -0.5, 0.5),
        "gate_bias": noise(arg_keys[4], (H * HD,), 1.0, 4.0, (), jnp.float32),
        "w_bias": draw_w_bias(jax.random.fold_in(arg_keys[9], 71), 0),
        "w_out": noise(arg_keys[6], (H * HD, C), (H * HD) ** -0.5, 0.5),
        "out_bias": noise(arg_keys[7], (C,), 0.5, 3.0, (), jnp.float32),
        "block_valid": draw_block_valid(jax.random.fold_in(arg_keys[9], 71), 0),
    }


def layer_norm(values, ln_gain, ln_shift):
    widened = values.astype(jnp.float32)
    average = lax.optimization_barrier(jnp.mean(widened, axis=-1, keepdims=True))
    spread = lax.optimization_barrier(jnp.mean((widened - average) ** 2, axis=-1, keepdims=True))
    return ((widened - average) * lax.rsqrt(spread + 1e-05) * ln_gain + ln_shift).astype(jnp.bfloat16)

def residue_valid(block_valid, residues):
    blocks = block_valid.shape[0]
    block_width = residues // blocks
    owner = jnp.arange(residues, dtype=jnp.int32) // block_width
    matches = (owner[:, None] == jnp.arange(blocks, dtype=jnp.int32)[None, :]).astype(jnp.float32)
    return lax.optimization_barrier(jnp.sum(matches * block_valid.astype(jnp.float32)[None, :], axis=1))

def reference(pair_rep, ln_gain, ln_shift, w_proj, gate_bias, w_bias, w_out, out_bias, block_valid):
    residues = pair_rep.shape[0]
    inner = H * HD
    validity = residue_valid(block_valid, residues)
    normed = lax.map(lambda row_in: layer_norm(row_in, ln_gain, ln_shift), pair_rep)
    bias_rows = lax.map(lambda row_in: jnp.dot(row_in, w_bias, preferred_element_type=jnp.float32), normed)
    bias_t = jnp.transpose(bias_rows, (2, 1, 0))

    def column(index):
        column_in = lax.dynamic_index_in_dim(normed, index, 1, keepdims=False)
        pair_col = lax.dynamic_index_in_dim(pair_rep, index, 1, keepdims=False)
        projected = jnp.dot(column_in, w_proj, preferred_element_type=jnp.float32)
        queries = (projected[:, :inner] * HD ** (-0.5)).astype(jnp.bfloat16)
        key_rows = projected[:, inner:2 * inner].astype(jnp.bfloat16)
        values = projected[:, 2 * inner:3 * inner].astype(jnp.bfloat16)
        gate_act = jax.nn.sigmoid(projected[:, 3 * inner:] + gate_bias)
        query_heads = queries.reshape(residues, H, HD).astype(jnp.float32)
        key_heads = key_rows.reshape(residues, H, HD).astype(jnp.float32)
        value_heads = values.reshape(residues, H, HD).astype(jnp.float32)
        scores = jnp.einsum('ihd,khd->hik', query_heads, key_heads) + bias_t
        scores = jnp.where(validity[None, None, :] > 0, scores, jnp.float32(-1e+30))
        row_max = lax.optimization_barrier(jnp.max(scores, axis=-1, keepdims=True))
        weights = jnp.exp(scores - row_max) * validity[None, None, :]
        denominator = lax.optimization_barrier(jnp.sum(weights, axis=-1))
        rounded = weights.astype(jnp.bfloat16).astype(jnp.float32)
        mixed = jnp.einsum('hik,khd->ihd', rounded, value_heads) / jnp.transpose(denominator)[:, :, None]
        attended = mixed.reshape(residues, inner).astype(jnp.bfloat16)
        gated_rows = (gate_act * attended.astype(jnp.float32)).astype(jnp.bfloat16)
        update = jnp.dot(gated_rows, w_out, preferred_element_type=jnp.float32) + out_bias
        col_valid = lax.dynamic_index_in_dim(validity, index, 0, keepdims=False)
        update = update * (validity * col_valid)[:, None]
        return (pair_col.astype(jnp.float32) + update).astype(jnp.bfloat16)
    results = lax.map(column, jnp.arange(residues, dtype=jnp.int32))
    return jnp.transpose(results, (1, 0, 2))
```

```python
import functools

import jax
import jax.numpy as jnp
from jax import lax
from jax.experimental import pallas as pl
from jax.experimental.pallas import tpu as pltpu
from jax.sharding import PartitionSpec as P

H = 4
HD = 32
NT = (((1,), (1,)), ((), ()))


def norm_kernel(pair_ref, gain_ref, shift_ref, wb_ref, normed_ref, bias_ref, held):
    rows, step_j, channels = pair_ref.shape
    flat = pair_ref[...].astype(jnp.float32).reshape(rows * step_j, channels)
    average = jnp.mean(flat, axis=-1, keepdims=True)
    centred = flat - average
    spread = jnp.mean(centred * centred, axis=-1, keepdims=True)
    held[...] = centred * lax.rsqrt(spread + 1e-05) * gain_ref[...] + shift_ref[...]
    for j in range(step_j):
        column = held[pl.ds(j, rows, stride=step_j), :].astype(jnp.bfloat16)
        normed_ref[j] = column
        part = lax.dot_general(wb_ref[...], column, NT, preferred_element_type=jnp.float32)
        for h in range(H):
            bias_ref[h, j : j + 1, :] = part[h : h + 1, :]


def attend_kernel(
    flags_ref, x_ref, w_ref, gb_ref, bias_ref, out_ref, order, q4, keys, vext, gates
):
    slots, _, rows, channels = x_ref.shape
    inner = H * HD
    tiles = rows // bias_ref.shape[3]
    count = jnp.int32(0)
    for b in range(slots):
        order[count] = b
        count = count + flags_ref[b]
    lane = lax.broadcasted_iota(jnp.int32, (rows, inner), 1) // HD

    def project(s, carry):
        x = x_ref[order[s], 0]
        proj = jnp.dot(x, w_ref[...], preferred_element_type=jnp.float32)
        q = proj[:, :inner] * HD ** (-0.5)
        for h in range(H):
            q4[s, h] = jnp.where(lane == h, q, 0.0).astype(jnp.bfloat16)
        at = pl.ds(pl.multiple_of(s * rows, rows), rows)
        keys[at, :] = proj[:, inner : 2 * inner].astype(jnp.bfloat16)
        vext[at, :inner] = proj[:, 2 * inner : 3 * inner].astype(jnp.bfloat16)
        vext[at, inner:] = jnp.ones((rows, inner), jnp.bfloat16)
        gates[s] = jax.nn.sigmoid(proj[:, 3 * inner :] + gb_ref[...])
        return carry

    wanted = count * flags_ref[slots]
    lax.fori_loop(0, wanted, project, 0)

    def queries(n):
        def body(s, carry):
            block = order[s]
            top = jnp.zeros((rows, inner), jnp.float32)
            low = jnp.ones((rows, inner), jnp.float32)
            for h in range(H):
                scores = lax.dot_general(
                    q4[s, h], keys[: n * rows, :], NT, preferred_element_type=jnp.float32
                )
                parts = [
                    bias_ref[order[t], pl.ds(block * tiles, tiles), h].reshape(rows, rows)
                    for t in range(n)
                ]
                scores = scores + jnp.concatenate(parts, axis=1)
                peak = jnp.max(scores, axis=-1, keepdims=True)
                weights = jnp.exp(scores - peak).astype(jnp.bfloat16)
                mixed = jnp.dot(weights, vext[: n * rows, :], preferred_element_type=jnp.float32)
                top = jnp.where(lane == h, mixed[:, :inner], top)
                low = jnp.where(lane == h, mixed[:, inner:], low)
            attended = (top / low).astype(jnp.bfloat16).astype(jnp.float32)
            out_ref[block, 0] = (gates[s] * attended).astype(jnp.bfloat16)
            return carry

        lax.fori_loop(0, wanted, body, 0)

    for n in range(1, keys.shape[0] // rows + 1):
        pl.when(count == n)(functools.partial(queries, n))


def close_kernel(flags_ref, gated_ref, pair_ref, w_ref, ob_ref, out_ref, held):
    cols, step_i, inner = gated_ref.shape

    @pl.when(flags_ref[0] > 0)
    def _():
        flat = gated_ref[...].reshape(cols * step_i, inner)
        held[...] = jnp.dot(flat, w_ref[...], preferred_element_type=jnp.float32) + ob_ref[...]
        for i in range(step_i):
            update = held[pl.ds(i, cols, stride=step_i), :]
            out_ref[i] = (pair_ref[i].astype(jnp.float32) + update).astype(jnp.bfloat16)

    @pl.when(flags_ref[0] == 0)
    def _():
        out_ref[...] = pair_ref[...]


def shards(pair_rep, ln_gain, ln_shift, w_proj, gate_bias, w_bias, w_out, out_bias, block_valid):
    rows, cols, channels = pair_rep.shape
    row_count = lax.axis_size("row")
    col_count = lax.axis_size("col")
    row_id = lax.axis_index("row")
    col_id = lax.axis_index("col")
    inner = H * HD
    width = cols // row_count
    blocks = block_valid.shape[0]
    block_width = rows * row_count // blocks
    assert block_width % rows == 0 and block_width % cols == 0 and rows % cols == 0
    most = row_count - block_width // rows
    smem = pl.BlockSpec(memory_space=pltpu.SMEM)

    def whole(*shape):
        return pl.BlockSpec(shape, lambda g: (0,) * len(shape))

    present = (block_valid > 0).astype(jnp.int32)
    per_slot = jnp.repeat(present, row_count // blocks) if row_count != blocks else present
    col_ok = present[col_id * cols // block_width]
    row_ok = present[row_id * rows // block_width]
    flags = jnp.concatenate([per_slot, col_ok[None]])
    own = (col_ok * row_ok)[None]

    step_j = 16 if cols % 16 == 0 else cols
    normed, bias_local = pl.pallas_call(
        norm_kernel,
        grid=(cols // step_j,),
        in_specs=[
            pl.BlockSpec((rows, step_j, channels), lambda g: (0, g, 0)),
            whole(1, channels),
            whole(1, channels),
            whole(H, channels),
        ],
        out_specs=[
            pl.BlockSpec((step_j, rows, channels), lambda g: (g, 0, 0)),
            pl.BlockSpec((H, step_j, rows), lambda g: (0, g, 0)),
        ],
        out_shape=[
            jax.ShapeDtypeStruct((cols, rows, channels), jnp.bfloat16),
            jax.ShapeDtypeStruct((H, cols, rows), jnp.float32),
        ],
        scratch_shapes=[pltpu.VMEM((rows * step_j, channels), jnp.float32)],
        name="norm",
    )(pair_rep, ln_gain[None], ln_shift[None], w_bias.T)

    bias = lax.all_gather(bias_local, ("row", "col"), axis=0)
    bias = bias.reshape(row_count, col_count, H, cols, rows)
    x = lax.all_to_all(
        normed.reshape(row_count, width, rows, channels), "row", 0, 0, tiled=True
    )
    gated = pl.pallas_call(
        attend_kernel,
        grid=(width,),
        in_specs=[
            smem,
            pl.BlockSpec((row_count, 1, rows, channels), lambda g: (0, g, 0, 0)),
            whole(channels, 4 * inner),
            whole(1, inner),
            pl.BlockSpec(
                (row_count, col_count, H, cols, rows),
                lambda g: (0, 0, 0, 0, 0),
                pipeline_mode=pl.Buffered(1),
            ),
        ],
        out_specs=pl.BlockSpec((row_count, 1, rows, inner), lambda g: (0, g, 0, 0)),
        out_shape=jax.ShapeDtypeStruct((row_count, width, rows, inner), jnp.bfloat16),
        scratch_shapes=[
            pltpu.SMEM((row_count + 1,), jnp.int32),
            pltpu.VMEM((most, H, rows, inner), jnp.bfloat16),
            pltpu.VMEM((most * rows, inner), jnp.bfloat16),
            pltpu.VMEM((most * rows, 2 * inner), jnp.bfloat16),
            pltpu.VMEM((most, rows, inner), jnp.float32),
        ],
        name="attend",
    )(flags, x, w_proj, gate_bias[None], bias)
    gated = lax.all_to_all(gated, "row", 0, 0, tiled=True)

    step_i = 32 if rows % 32 == 0 else rows
    return pl.pallas_call(
        close_kernel,
        grid=(rows // step_i,),
        in_specs=[
            smem,
            pl.BlockSpec((cols, step_i, inner), lambda g: (0, g, 0)),
            pl.BlockSpec((step_i, cols, channels), lambda g: (g, 0, 0)),
            whole(inner, channels),
            whole(1, channels),
        ],
        out_specs=pl.BlockSpec((step_i, cols, channels), lambda g: (g, 0, 0)),
        out_shape=jax.ShapeDtypeStruct((rows, cols, channels), jnp.bfloat16),
        scratch_shapes=[pltpu.VMEM((cols * step_i, channels), jnp.float32)],
        name="close",
    )(own, gated.reshape(cols, rows, inner), pair_rep, w_out, out_bias[None])


def solution(mesh):
    return jax.shard_map(
        shards,
        mesh=mesh,
        in_specs=(P("row", "col", None), P(), P(), P(), P(), P(), P(), P(), P()),
        out_specs=P("row", "col", None),
        check_vma=False,
    )
```

```python
import functools

import jax
import jax.numpy as jnp
from jax import lax
from jax.experimental import pallas as pl
from jax.experimental.pallas import tpu as pltpu
from jax.sharding import PartitionSpec as P

H = 4
HD = 32
NT = (((1,), (1,)), ((), ()))


def norm_kernel(pair_ref, gain_ref, shift_ref, wb_ref, normed_ref, bias_ref, held):
    rows, step_j, channels = pair_ref.shape
    flat = pair_ref[...].astype(jnp.float32).reshape(rows * step_j, channels)
    average = jnp.mean(flat, axis=-1, keepdims=True)
    centred = flat - average
    spread = jnp.mean(centred * centred, axis=-1, keepdims=True)
    held[...] = centred * lax.rsqrt(spread + 1e-05) * gain_ref[...] + shift_ref[...]
    for j in range(step_j):
        column = held[pl.ds(j, rows, stride=step_j), :].astype(jnp.bfloat16)
        normed_ref[j] = column
        part = lax.dot_general(wb_ref[...], column, NT, preferred_element_type=jnp.float32)
        for h in range(H):
            bias_ref[h, j : j + 1, :] = part[h : h + 1, :]


def attend_kernel(
    flags_ref, x_ref, w_ref, gb_ref, bias_ref, out_ref, order, q4, keys, vext, gates
):
    slots, _, rows, channels = x_ref.shape
    inner = H * HD
    tiles = rows // bias_ref.shape[3]
    count = jnp.int32(0)
    for b in range(slots):
        order[count] = b
        count = count + flags_ref[b]
    lane = lax.broadcasted_iota(jnp.int32, (rows, inner), 1) // HD

    def project(s):
        x = x_ref[order[s], 0]
        proj = jnp.dot(x, w_ref[...], preferred_element_type=jnp.float32)
        q = proj[:, :inner] * HD ** (-0.5)
        for h in range(H):
            q4[s, h] = jnp.where(lane == h, q, 0.0).astype(jnp.bfloat16)
        at = pl.ds(s * rows, rows)
        keys[at, :] = proj[:, inner : 2 * inner].astype(jnp.bfloat16)
        vext[at, :inner] = proj[:, 2 * inner : 3 * inner].astype(jnp.bfloat16)
        vext[at, inner:] = jnp.ones((rows, inner), jnp.bfloat16)
        gates[s] = jax.nn.sigmoid(proj[:, 3 * inner :] + gb_ref[...])

    def score(n, s, h):
        parts = [
            bias_ref[pl.ds(order[s] * tiles, tiles), order[t], h].reshape(rows, rows)
            for t in range(n)
        ]
        scores = lax.dot_general(
            q4[s, h], keys[: n * rows, :], NT, preferred_element_type=jnp.float32
        )
        return scores + jnp.concatenate(parts, axis=1)

    def queries(n, members):
        jobs = [(s, h) for s in members for h in range(H)]
        scores = [score(n, s, h) for s, h in jobs]
        peaks = [jnp.max(v, axis=-1, keepdims=True) for v in scores]
        weights = [jnp.exp(v - p).astype(jnp.bfloat16) for v, p in zip(scores, peaks)]
        mixed = [
            jnp.dot(w, vext[: n * rows, :], preferred_element_type=jnp.float32) for w in weights
        ]
        for at, s in enumerate(members):
            heads = mixed[at * H : (at + 1) * H]
            top, low = heads[0][:, :inner], heads[0][:, inner:]
            for h in range(1, H):
                top = jnp.where(lane == h, heads[h][:, :inner], top)
                low = jnp.where(lane == h, heads[h][:, inner:], low)
            attended = (top / low).astype(jnp.bfloat16).astype(jnp.float32)
            out_ref[order[s], 0] = (gates[s] * attended).astype(jnp.bfloat16)

    def column(n):
        for s in range(n):
            project(s)
        group = max(1, 9 // n)
        for first in range(0, n, group):
            queries(n, list(range(first, min(n, first + group))))

    wanted = count * flags_ref[slots]
    for n in range(1, keys.shape[0] // rows + 1):
        pl.when(wanted == n)(functools.partial(column, n))


def swap_kernel(
    x_ref, bias_ref, y_ref, all_ref, stage, local_sem, bs, br, xs, xr, us, ur, ds, dr, ps, pr
):
    row_count = x_ref.shape[0]
    col_count = all_ref.shape[0]
    lines = col_count // 2
    row = lax.axis_index("row")
    col = lax.axis_index("col")
    u = col // 2
    core = col - 2 * u
    twin = 2 * u + 1 - core

    def to(ref_from, ref_to, send, recv, r, c):
        return pltpu.make_async_remote_copy(
            src_ref=ref_from,
            dst_ref=ref_to,
            send_sem=send,
            recv_sem=recv,
            device_id=(r, c),
            device_id_type=pl.DeviceIdType.MESH,
        )

    barrier = pltpu.get_barrier_semaphore()

    def greet(r, c):
        pl.semaphore_signal(
            barrier, inc=1, device_id=(r, c), device_id_type=pl.DeviceIdType.MESH
        )

    mine = pltpu.make_async_copy(bias_ref, all_ref.at[col, row], local_sem.at[0])
    load = pltpu.make_async_copy(x_ref.at[row], stage, local_sem.at[1])
    mine.start()
    load.start()
    for d in range(1, row_count):
        greet(lax.rem(row + d, row_count), col)
    greet(row, twin)
    pl.when(u > 0)(lambda: greet(row, col - 2))
    pl.when(u + 1 < lines)(lambda: greet(row, col + 2))
    ends = jnp.where(u > 0, 1, 0) + jnp.where(u + 1 < lines, 1, 0)
    pl.semaphore_wait(barrier, row_count + ends)

    pieces, chunks = [], []
    for d in range(1, row_count):
        peer = lax.rem(row + d, row_count)
        piece = to(bias_ref, all_ref.at[col, row], bs.at[d - 1], br.at[d - 1], peer, col)
        piece.start()
        pieces.append(piece)
    for d in range(1, row_count):
        peer = lax.rem(row + d, row_count)
        chunk = to(x_ref.at[peer], y_ref.at[row], xs.at[d - 1], xr.at[d - 1], peer, col)
        chunk.start()
        chunks.append(chunk)
    load.wait()
    keep = pltpu.make_async_copy(stage, y_ref.at[row], local_sem.at[1])
    keep.start()
    mine.wait()
    for d in range(1, row_count):
        origin = lax.rem(row - d + row_count, row_count)
        to(
            bias_ref, all_ref.at[col, origin], bs.at[d - 1], br.at[d - 1], origin, col
        ).wait_recv()

    def up(t):
        block = all_ref.at[col - 2 * t]
        return to(block, block, us.at[t], ur.at[t], row, col + 2)

    def down(t):
        block = all_ref.at[col + 2 * t]
        return to(block, block, ds.at[t], dr.at[t], row, col - 2)

    def across(t, sign):
        block = all_ref.at[col + sign * 2 * t]
        return to(block, block, ps.at[u + sign * t], pr.at[u + sign * t], row, twin)

    for t in range(lines):

        @pl.when(u - t >= 0)
        def _():
            if t > 0:
                block = all_ref.at[col - 2 * t]
                to(block, block, us.at[t - 1], ur.at[t - 1], row, col - 2).wait_recv()
            pl.when(u + 1 < lines)(lambda: up(t).start())
            across(t, -1).start()

        @pl.when(u + t < lines)
        def _():
            if t > 0:
                block = all_ref.at[col + 2 * t]
                to(block, block, ds.at[t - 1], dr.at[t - 1], row, col + 2).wait_recv()
            pl.when(u > 0)(lambda: down(t).start())
            if t > 0:
                across(t, 1).start()

    for d in range(1, row_count):
        origin = lax.rem(row - d + row_count, row_count)
        pieces[d - 1].wait_send()
        chunks[d - 1].wait_send()
        to(
            x_ref.at[origin], y_ref.at[origin], xs.at[d - 1], xr.at[d - 1], origin, col
        ).wait_recv()
    keep.wait()
    for t in range(lines):

        @pl.when(u - t >= 0)
        def _():
            pl.when(u + 1 < lines)(lambda: up(t).wait_send())
            across(t, -1).wait_send()

        @pl.when(u + t < lines)
        def _():
            pl.when(u > 0)(lambda: down(t).wait_send())
            if t > 0:
                across(t, 1).wait_send()

    for p in range(lines):
        block = all_ref.at[2 * p + 1 - core]
        to(block, block, ps.at[p], pr.at[p], row, twin).wait_recv()


def close_kernel(flags_ref, gated_ref, pair_ref, w_ref, ob_ref, out_ref, held):
    cols, step_i, inner = gated_ref.shape

    @pl.when(flags_ref[0] > 0)
    def _():
        flat = gated_ref[...].reshape(cols * step_i, inner)
        held[...] = jnp.dot(flat, w_ref[...], preferred_element_type=jnp.float32) + ob_ref[...]
        for i in range(step_i):
            update = held[pl.ds(i, cols, stride=step_i), :]
            out_ref[i] = (pair_ref[i].astype(jnp.float32) + update).astype(jnp.bfloat16)

    @pl.when(flags_ref[0] == 0)
    def _():
        out_ref[...] = pair_ref[...]


def shards(pair_rep, ln_gain, ln_shift, w_proj, gate_bias, w_bias, w_out, out_bias, block_valid):
    rows, cols, channels = pair_rep.shape
    row_count = lax.axis_size("row")
    col_count = lax.axis_size("col")
    row_id = lax.axis_index("row")
    col_id = lax.axis_index("col")
    inner = H * HD
    width = cols // row_count
    blocks = block_valid.shape[0]
    block_width = rows * row_count // blocks
    assert block_width % rows == 0 and block_width % cols == 0 and rows % cols == 0
    most = row_count - block_width // rows
    smem = pl.BlockSpec(memory_space=pltpu.SMEM)

    def whole(*shape):
        return pl.BlockSpec(shape, lambda g: (0,) * len(shape))

    present = (block_valid > 0).astype(jnp.int32)
    per_slot = jnp.repeat(present, row_count // blocks) if row_count != blocks else present
    col_ok = present[col_id * cols // block_width]
    row_ok = present[row_id * rows // block_width]
    flags = jnp.concatenate([per_slot, col_ok[None]])
    own = (col_ok * row_ok)[None]

    step_j = 16 if cols % 16 == 0 else cols
    normed, bias_local = pl.pallas_call(
        norm_kernel,
        grid=(cols // step_j,),
        in_specs=[
            pl.BlockSpec((rows, step_j, channels), lambda g: (0, g, 0)),
            whole(1, channels),
            whole(1, channels),
            whole(H, channels),
        ],
        out_specs=[
            pl.BlockSpec((step_j, rows, channels), lambda g: (g, 0, 0)),
            pl.BlockSpec((H, step_j, rows), lambda g: (0, g, 0)),
        ],
        out_shape=[
            jax.ShapeDtypeStruct((cols, rows, channels), jnp.bfloat16),
            jax.ShapeDtypeStruct((H, cols, rows), jnp.float32),
        ],
        scratch_shapes=[pltpu.VMEM((rows * step_j, channels), jnp.float32)],
        name="norm",
    )(pair_rep, ln_gain[None], ln_shift[None], w_bias.T)

    lines = col_count // 2
    sems = pltpu.SemaphoreType.DMA
    x, bias = pl.pallas_call(
        swap_kernel,
        in_specs=[
            pl.BlockSpec(memory_space=pl.ANY),
            pl.BlockSpec(memory_space=pltpu.VMEM),
        ],
        out_specs=[pl.BlockSpec(memory_space=pl.ANY)] * 2,
        out_shape=[
            jax.ShapeDtypeStruct((row_count, width, rows, channels), jnp.bfloat16),
            jax.ShapeDtypeStruct((col_count, row_count, H, cols, rows), jnp.float32),
        ],
        scratch_shapes=[pltpu.VMEM((width, rows, channels), jnp.bfloat16), sems((2,))]
        + [sems((row_count - 1,))] * 4
        + [sems((lines,))] * 6,
        compiler_params=pltpu.CompilerParams(collective_id=0, has_side_effects=True),
        name="swap",
    )(normed.reshape(row_count, width, rows, channels), bias_local)
    gated = pl.pallas_call(
        attend_kernel,
        grid=(width,),
        in_specs=[
            smem,
            pl.BlockSpec((row_count, 1, rows, channels), lambda g: (0, g, 0, 0)),
            whole(channels, 4 * inner),
            whole(1, inner),
            pl.BlockSpec(
                (col_count, row_count, H, cols, rows),
                lambda g: (0, 0, 0, 0, 0),
                pipeline_mode=pl.Buffered(1),
            ),
        ],
        out_specs=pl.BlockSpec((row_count, 1, rows, inner), lambda g: (0, g, 0, 0)),
        out_shape=jax.ShapeDtypeStruct((row_count, width, rows, inner), jnp.bfloat16),
        scratch_shapes=[
            pltpu.SMEM((row_count + 1,), jnp.int32),
            pltpu.VMEM((most, H, rows, inner), jnp.bfloat16),
            pltpu.VMEM((most * rows, inner), jnp.bfloat16),
            pltpu.VMEM((most * rows, 2 * inner), jnp.bfloat16),
            pltpu.VMEM((most, rows, inner), jnp.float32),
        ],
        name="attend",
    )(flags, x, w_proj, gate_bias[None], bias)
    gated = lax.all_to_all(gated, "row", 0, 0, tiled=True)

    step_i = 32 if rows % 32 == 0 else rows
    return pl.pallas_call(
        close_kernel,
        grid=(rows // step_i,),
        in_specs=[
            smem,
            pl.BlockSpec((cols, step_i, inner), lambda g: (0, g, 0)),
            pl.BlockSpec((step_i, cols, channels), lambda g: (g, 0, 0)),
            whole(inner, channels),
            whole(1, channels),
        ],
        out_specs=pl.BlockSpec((step_i, cols, channels), lambda g: (g, 0, 0)),
        out_shape=jax.ShapeDtypeStruct((rows, cols, channels), jnp.bfloat16),
        scratch_shapes=[pltpu.VMEM((cols * step_i, channels), jnp.float32)],
        name="close",
    )(own, gated.reshape(cols, rows, inner), pair_rep, w_out, out_bias[None])


def solution(mesh):
    return jax.shard_map(
        shards,
        mesh=mesh,
        in_specs=(P("row", "col", None), P(), P(), P(), P(), P(), P(), P(), P()),
        out_specs=P("row", "col", None),
        check_vma=False,
    )
```

```python
import functools

import jax
import jax.numpy as jnp
from jax import lax
from jax.experimental import pallas as pl
from jax.experimental.pallas import tpu as pltpu
from jax.sharding import PartitionSpec as P

H = 4
HD = 32
NT = (((1,), (1,)), ((), ()))


def norm_kernel(pair_ref, gain_ref, shift_ref, wb_ref, normed_ref, bias_ref, held):
    rows, step_j, channels = pair_ref.shape
    flat = pair_ref[...].astype(jnp.float32).reshape(rows * step_j, channels)
    average = jnp.mean(flat, axis=-1, keepdims=True)
    centred = flat - average
    spread = jnp.mean(centred * centred, axis=-1, keepdims=True)
    held[...] = centred * lax.rsqrt(spread + 1e-05) * gain_ref[...] + shift_ref[...]
    for j in range(step_j):
        column = held[pl.ds(j, rows, stride=step_j), :].astype(jnp.bfloat16)
        normed_ref[j] = column
        part = lax.dot_general(wb_ref[...], column, NT, preferred_element_type=jnp.float32)
        for h in range(H):
            bias_ref[h, j : j + 1, :] = part[h : h + 1, :]


def attend_kernel(
    flags_ref, x_ref, w_ref, gb_ref, bias_ref, out_ref, order, q4, keys, vext, gates
):
    slots, _, rows, channels = x_ref.shape
    inner = H * HD
    tiles = rows // bias_ref.shape[3]
    count = jnp.int32(0)
    for b in range(slots):
        order[count] = b
        count = count + flags_ref[b]
    lane = lax.broadcasted_iota(jnp.int32, (rows, inner), 1) // HD

    def project(s):
        x = x_ref[order[s], 0]
        proj = jnp.dot(x, w_ref[...], preferred_element_type=jnp.float32)
        q = proj[:, :inner] * HD ** (-0.5)
        for h in range(H):
            q4[s, h] = jnp.where(lane == h, q, 0.0).astype(jnp.bfloat16)
        at = pl.ds(s * rows, rows)
        keys[at, :] = proj[:, inner : 2 * inner].astype(jnp.bfloat16)
        vext[at, :inner] = proj[:, 2 * inner : 3 * inner].astype(jnp.bfloat16)
        vext[at, inner:] = jnp.ones((rows, inner), jnp.bfloat16)
        gates[s] = jax.nn.sigmoid(proj[:, 3 * inner :] + gb_ref[...])

    def score(n, s, h):
        parts = [
            bias_ref[pl.ds(order[s] * tiles, tiles), lax.rem(order[t] + flags_ref[slots + 1], slots), h].reshape(rows, rows)
            for t in range(n)
        ]
        scores = lax.dot_general(
            q4[s, h], keys[: n * rows, :], NT, preferred_element_type=jnp.float32
        )
        return scores + jnp.concatenate(parts, axis=1)

    def queries(n, members):
        jobs = [(s, h) for s in members for h in range(H)]
        scores = [score(n, s, h) for s, h in jobs]
        peaks = [jnp.max(v, axis=-1, keepdims=True) for v in scores]
        weights = [jnp.exp(v - p).astype(jnp.bfloat16) for v, p in zip(scores, peaks)]
        mixed = [
            jnp.dot(w, vext[: n * rows, :], preferred_element_type=jnp.float32) for w in weights
        ]
        for at, s in enumerate(members):
            heads = mixed[at * H : (at + 1) * H]
            top, low = heads[0][:, :inner], heads[0][:, inner:]
            for h in range(1, H):
                top = jnp.where(lane == h, heads[h][:, :inner], top)
                low = jnp.where(lane == h, heads[h][:, inner:], low)
            attended = (top / low).astype(jnp.bfloat16).astype(jnp.float32)
            out_ref[order[s], 0] = (gates[s] * attended).astype(jnp.bfloat16)

    def column(n):
        for s in range(n):
            project(s)
        group = max(1, 9 // n)
        for first in range(0, n, group):
            queries(n, list(range(first, min(n, first + group))))

    wanted = count * flags_ref[slots]
    for n in range(1, keys.shape[0] // rows + 1):
        pl.when(wanted == n)(functools.partial(column, n))


def swap_kernel(
    skip, x_ref, bias_ref, y_ref, all_ref, stage, local_sem, bs, br, xs, xr, us, ur, ds, dr, ps, pr
):
    row_count = x_ref.shape[0]
    col_count = all_ref.shape[0]
    lines = col_count // 2
    row = lax.axis_index("row")
    col = lax.axis_index("col")
    u = col // 2
    core = col - 2 * u
    twin = 2 * u + 1 - core

    def slot(r):
        return lax.rem(r + row_count - 1 - skip, row_count)

    cols, rows = bias_ref.shape[1:]
    fine = [p for p in range(lines) if p * 2 * cols // rows != skip]
    top = fine[-1]

    def below(t):
        v = u - t
        return (v >= 0) & (lax.div(v * 2 * cols, rows) != skip) & (u <= top)

    def above(t):
        v = u + t
        return (v < lines) & (lax.div(v * 2 * cols, rows) != skip)

    def block_of(c):
        return all_ref.at[c, pl.ds(0, row_count - 1)]

    def to(ref_from, ref_to, send, recv, r, c):
        return pltpu.make_async_remote_copy(
            src_ref=ref_from,
            dst_ref=ref_to,
            send_sem=send,
            recv_sem=recv,
            device_id=(r, c),
            device_id_type=pl.DeviceIdType.MESH,
        )

    barrier = pltpu.get_barrier_semaphore()

    def greet(r, c):
        pl.semaphore_signal(
            barrier, inc=1, device_id=(r, c), device_id_type=pl.DeviceIdType.MESH
        )

    mine = pltpu.make_async_copy(bias_ref, all_ref.at[col, slot(row)], local_sem.at[0])
    load = pltpu.make_async_copy(x_ref.at[row], stage, local_sem.at[1])
    mine.start()
    load.start()
    for d in range(1, row_count):
        greet(lax.rem(row + d, row_count), col)
    greet(row, twin)
    pl.when(u > 0)(lambda: greet(row, col - 2))
    pl.when(u + 1 < lines)(lambda: greet(row, col + 2))
    ends = jnp.where(u > 0, 1, 0) + jnp.where(u + 1 < lines, 1, 0)
    pl.semaphore_wait(barrier, row_count + ends)

    pieces, chunks = [], []
    for d in range(1, row_count):
        peer = lax.rem(row + d, row_count)
        piece = to(bias_ref, all_ref.at[col, slot(row)], bs.at[d - 1], br.at[d - 1], peer, col)
        piece.start()
        pieces.append(piece)
    for d in range(1, row_count):
        peer = lax.rem(row + d, row_count)
        chunk = to(x_ref.at[peer], y_ref.at[row], xs.at[d - 1], xr.at[d - 1], peer, col)
        chunk.start()
        chunks.append(chunk)
    load.wait()
    keep = pltpu.make_async_copy(stage, y_ref.at[row], local_sem.at[1])
    keep.start()
    mine.wait()
    for d in range(1, row_count):
        origin = lax.rem(row - d + row_count, row_count)
        to(
            bias_ref, all_ref.at[col, slot(origin)], bs.at[d - 1], br.at[d - 1], origin, col
        ).wait_recv()

    def up(t):
        block = block_of(col - 2 * t)
        return to(block, block, us.at[t], ur.at[t], row, col + 2)

    def down(t):
        block = block_of(col + 2 * t)
        return to(block, block, ds.at[t], dr.at[t], row, col - 2)

    def across(t, sign):
        block = block_of(col + sign * 2 * t)
        return to(block, block, ps.at[u + sign * t], pr.at[u + sign * t], row, twin)

    for t in range(lines):

        @pl.when(below(t))
        def _():
            if t > 0:
                block = block_of(col - 2 * t)
                to(block, block, us.at[t - 1], ur.at[t - 1], row, col - 2).wait_recv()
            pl.when(u < top)(lambda: up(t).start())
            across(t, -1).start()

        @pl.when(above(t))
        def _():
            if t > 0:
                block = block_of(col + 2 * t)
                to(block, block, ds.at[t - 1], dr.at[t - 1], row, col + 2).wait_recv()
            pl.when(u > 0)(lambda: down(t).start())
            if t > 0:
                across(t, 1).start()

    for d in range(1, row_count):
        origin = lax.rem(row - d + row_count, row_count)
        pieces[d - 1].wait_send()
        chunks[d - 1].wait_send()
        to(
            x_ref.at[origin], y_ref.at[origin], xs.at[d - 1], xr.at[d - 1], origin, col
        ).wait_recv()
    keep.wait()
    for t in range(lines):

        @pl.when(below(t))
        def _():
            pl.when(u < top)(lambda: up(t).wait_send())
            across(t, -1).wait_send()

        @pl.when(above(t))
        def _():
            pl.when(u > 0)(lambda: down(t).wait_send())
            if t > 0:
                across(t, 1).wait_send()

    @pl.when(u <= top)
    def _():
        for p in fine:
            block = block_of(2 * p + 1 - core)
            to(block, block, ps.at[p], pr.at[p], row, twin).wait_recv()


def close_kernel(flags_ref, gated_ref, pair_ref, w_ref, ob_ref, out_ref, held):
    cols, step_i, inner = gated_ref.shape

    @pl.when(flags_ref[0] > 0)
    def _():
        flat = gated_ref[...].reshape(cols * step_i, inner)
        held[...] = jnp.dot(flat, w_ref[...], preferred_element_type=jnp.float32) + ob_ref[...]
        for i in range(step_i):
            update = held[pl.ds(i, cols, stride=step_i), :]
            out_ref[i] = (pair_ref[i].astype(jnp.float32) + update).astype(jnp.bfloat16)

    @pl.when(flags_ref[0] == 0)
    def _():
        out_ref[...] = pair_ref[...]


def shards(pair_rep, ln_gain, ln_shift, w_proj, gate_bias, w_bias, w_out, out_bias, block_valid):
    rows, cols, channels = pair_rep.shape
    row_count = lax.axis_size("row")
    col_count = lax.axis_size("col")
    row_id = lax.axis_index("row")
    col_id = lax.axis_index("col")
    inner = H * HD
    width = cols // row_count
    blocks = block_valid.shape[0]
    block_width = rows * row_count // blocks
    assert block_width == rows and block_width % cols == 0 and rows % cols == 0
    most = row_count - block_width // rows
    smem = pl.BlockSpec(memory_space=pltpu.SMEM)

    def whole(*shape):
        return pl.BlockSpec(shape, lambda g: (0,) * len(shape))

    present = (block_valid > 0).astype(jnp.int32)
    per_slot = jnp.repeat(present, row_count // blocks) if row_count != blocks else present
    col_ok = present[col_id * cols // block_width]
    row_ok = present[row_id * rows // block_width]
    skip = jnp.argmin(present).astype(jnp.int32)
    flags = jnp.concatenate([per_slot, jnp.stack([col_ok, row_count - 1 - skip])])
    own = (col_ok * row_ok)[None]

    step_j = 16 if cols % 16 == 0 else cols
    normed, bias_local = pl.pallas_call(
        norm_kernel,
        grid=(cols // step_j,),
        in_specs=[
            pl.BlockSpec((rows, step_j, channels), lambda g: (0, g, 0)),
            whole(1, channels),
            whole(1, channels),
            whole(H, channels),
        ],
        out_specs=[
            pl.BlockSpec((step_j, rows, channels), lambda g: (g, 0, 0)),
            pl.BlockSpec((H, step_j, rows), lambda g: (0, g, 0)),
        ],
        out_shape=[
            jax.ShapeDtypeStruct((cols, rows, channels), jnp.bfloat16),
            jax.ShapeDtypeStruct((H, cols, rows), jnp.float32),
        ],
        scratch_shapes=[pltpu.VMEM((rows * step_j, channels), jnp.float32)],
        name="norm",
    )(pair_rep, ln_gain[None], ln_shift[None], w_bias.T)

    lines = col_count // 2
    sems = pltpu.SemaphoreType.DMA

    def swap(place, padded):
        return pl.pallas_call(
            functools.partial(swap_kernel, padded),
            in_specs=[
                pl.BlockSpec(memory_space=pl.ANY),
                pl.BlockSpec(memory_space=pltpu.VMEM),
            ],
            out_specs=[pl.BlockSpec(memory_space=pl.ANY)] * 2,
            out_shape=[
                jax.ShapeDtypeStruct((row_count, width, rows, channels), jnp.bfloat16),
                jax.ShapeDtypeStruct((col_count, row_count, H, cols, rows), jnp.float32),
            ],
            scratch_shapes=[pltpu.VMEM((width, rows, channels), jnp.bfloat16), sems((2,))]
            + [sems((row_count - 1,))] * 4
            + [sems((lines,))] * 6,
            compiler_params=pltpu.CompilerParams(collective_id=place, has_side_effects=True),
            name="swap",
        )

    options = [b for b in range(1, blocks) if b != blocks // 2]
    choice = sum((skip > b).astype(jnp.int32) for b in options[:-1])
    x, bias = lax.switch(
        choice,
        [swap(place, padded) for place, padded in enumerate(options)],
        normed.reshape(row_count, width, rows, channels),
        bias_local,
    )
    gated = pl.pallas_call(
        attend_kernel,
        grid=(width,),
        in_specs=[
            smem,
            pl.BlockSpec((row_count, 1, rows, channels), lambda g: (0, g, 0, 0)),
            whole(channels, 4 * inner),
            whole(1, inner),
            pl.BlockSpec(
                (col_count, row_count, H, cols, rows),
                lambda g: (0, 0, 0, 0, 0),
                pipeline_mode=pl.Buffered(1),
            ),
        ],
        out_specs=pl.BlockSpec((row_count, 1, rows, inner), lambda g: (0, g, 0, 0)),
        out_shape=jax.ShapeDtypeStruct((row_count, width, rows, inner), jnp.bfloat16),
        scratch_shapes=[
            pltpu.SMEM((row_count + 1,), jnp.int32),
            pltpu.VMEM((most, H, rows, inner), jnp.bfloat16),
            pltpu.VMEM((most * rows, inner), jnp.bfloat16),
            pltpu.VMEM((most * rows, 2 * inner), jnp.bfloat16),
            pltpu.VMEM((most, rows, inner), jnp.float32),
        ],
        name="attend",
    )(flags, x, w_proj, gate_bias[None], bias)
    gated = lax.all_to_all(gated, "row", 0, 0, tiled=True)

    step_i = 32 if rows % 32 == 0 else rows
    return pl.pallas_call(
        close_kernel,
        grid=(rows // step_i,),
        in_specs=[
            smem,
            pl.BlockSpec((cols, step_i, inner), lambda g: (0, g, 0)),
            pl.BlockSpec((step_i, cols, channels), lambda g: (g, 0, 0)),
            whole(inner, channels),
            whole(1, channels),
        ],
        out_specs=pl.BlockSpec((step_i, cols, channels), lambda g: (g, 0, 0)),
        out_shape=jax.ShapeDtypeStruct((rows, cols, channels), jnp.bfloat16),
        scratch_shapes=[pltpu.VMEM((cols * step_i, channels), jnp.float32)],
        name="close",
    )(own, gated.reshape(cols, rows, inner), pair_rep, w_out, out_bias[None])


def solution(mesh):
    return jax.shard_map(
        shards,
        mesh=mesh,
        in_specs=(P("row", "col", None), P(), P(), P(), P(), P(), P(), P(), P()),
        out_specs=P("row", "col", None),
        check_vma=False,
    )
```
